32 devices in a mesh: pipe: 1, seq: 32 (over z, y, x, core).
Axes of the slice: x: 2, y: 2, z: 4, core: 2. Of those that a mesh axis runs over, the one named last changes fastest.
Arguments:
- inputs: bfloat16 [2, 16384, 512], P(None, 'seq'), may hold values from -6 to 6
- w_in: bfloat16 [1, 512, 2048], P('pipe'), may hold values from -0.25 to 0.25
- w_out: bfloat16 [1, 512, 512], P('pipe'), may hold values from -0.25 to 0.25
- lengths: int32 [2, 8], replicated, may hold values from 1 to 4096, 16384 in all within a row
- valid: int32 [2, 32], replicated, may hold values from 128 to 512
Outputs:
- states: bfloat16 [1, 2, 16384, 512], P('pipe', None, 'seq')
The draws below stay inside these ranges and needn't reach their ends.
Inputs may be any that keep to these rules, and one draw needn't show every extreme that they name: Each row of stream lengths sums to 16384.
All inputs are finite; a program needn't handle non-finite values.
Results may differ from the reference program's by a relative error of at most 0.025.
Values may be sent and summed in bfloat16 or wider, within the bound.
No kernel may reach another device: no remote copies, remote signals or barrier semaphores. Data moves between devices by JAX's collectives and lax.ppermute only.
A program may use at most 64 MiB of HBM per device.

```python
import math
import jax
import jax.numpy as jnp
import numpy as np
from jax import lax

D = 512
HEADS = 4
HEAD_DIM = 128
WINDOW = 512
MICRO = 2
TOK_DEV = 512
HD = 512
LAYERS = 1
ROWS = 16384
GROUPS = 32
STREAMS = 8


def place_ends(array, stream_key, low, top_value):
    longest = array.shape.index(max(array.shape))
    spots = []
    for shift in (0, 1):
        where = [jax.random.randint(jax.random.fold_in(stream_key, axis), (), 0, length) for axis, length in enumerate(array.shape)]
        where[longest] = (where[longest] + shift) % array.shape[longest]
        spots.append(tuple(where))
    return array.at[spots[0]].set(low).at[spots[1]].set(top_value)


def steps_of(own_key, shape, pieces, smallest, top_value):
    factor_of = 1.0
    for axis_at, shards_of in pieces:
        steps = jax.random.uniform(jax.random.fold_in(jax.random.fold_in(own_key, 6), axis_at), (shards_of,), jnp.float32, smallest / len(pieces), top_value / len(pieces))
        factor_of = factor_of * jnp.repeat(jnp.exp(steps), shape[axis_at] // shards_of).reshape((-1,) + (1,) * (len(shape) - 1 - axis_at))
    return factor_of


def profile(number_of, total, limit, slope):
    portions = [(1 << 20) // math.isqrt(grade ** slope) + 1 for grade in range(2, number_of + 1)]
    surplus, holding = total - limit - (number_of - 1), [1] * (number_of - 1)
    while surplus > 0:
        candidates = [i for i in range(number_of - 1) if holding[i] < limit]
        pool, left = sum([portions[i] for i in candidates]), surplus
        for i in candidates:
            extra = min(limit - holding[i], max(1, left * portions[i] // pool), surplus)
            holding[i] = holding[i] + extra
            surplus = surplus - extra
    return np.array([limit] + holding)


def uneven(key, count, total, reach, skew):
    if count == 2:
        one = jax.random.randint(key, (), max(1, total - reach), min(reach, total - 1) + 1)
        return jnp.stack([one, total - one])
    tallies = jnp.asarray(profile(count, total, reach, skew), jnp.int32)
    pairs = (count - 1) // 2
    donor, sink = tallies[1:1 + 2 * pairs:2], tallies[2:2 + 2 * pairs:2]
    slack = jnp.minimum(donor - 1, reach - sink)
    moved = jax.random.randint(jax.random.fold_in(key, 1), (pairs,), 0, 1 << 20) % (slack + 1)
    tallies = tallies.at[1:1 + 2 * pairs:2].set(donor - moved).at[2:2 + 2 * pairs:2].set(sink + moved)
    return tallies[jax.random.permutation(jax.random.fold_in(key, 2), count)]


def scatter_about(key, shape, scale, bound, cuts=(), held_as=jnp.bfloat16):
    entries = jax.random.normal(key, shape, jnp.float32) * scale
    if len(cuts) > 0:
        entries = steps_of(key, shape, cuts, -0.22, 0.18) * entries
    return jnp.clip(entries, min=-bound, max=bound).astype(held_as)


def setup_inputs(seed: int = 0) -> dict:
    splits = jax.random.split(jax.random.key(seed), 6)
    return {
        "inputs": scatter_about(splits[0], (MICRO, ROWS, D), 1.0, 6.0, ((1, 32),)),
        "w_in": scatter_about(splits[1], (LAYERS, D, 4 * HD), D ** -0.5, 0.25),
        "w_out": scatter_about(splits[2], (LAYERS, HD, D), HD ** -0.5, 0.25),
        "lengths": jax.vmap(lambda own: uneven(own, STREAMS, ROWS, ROWS // 4, 2))(jax.random.split(splits[3], MICRO)).reshape((MICRO, STREAMS)).astype(jnp.int32),
        "valid": place_ends(jax.random.randint(splits[4], (MICRO, GROUPS), TOK_DEV // 4, TOK_DEV + 1), jax.random.fold_in(splits[4], 1), TOK_DEV // 4, TOK_DEV).astype(jnp.int32),
    }


norm_eps = 1e-05
out_eps = 0.001

def layer_norm(values, epsilon):
    mean = lax.optimization_barrier(jnp.mean(values, axis=-1, keepdims=True))
    centred = values - mean
    spread = lax.optimization_barrier(jnp.mean(centred * centred, axis=-1, keepdims=True))
    return centred / jnp.sqrt(spread + epsilon)

def one_layer(hidden, weight_in, weight_out, bounds, valid_row):
    rows = hidden.shape[0]
    width = HEADS * HEAD_DIM
    normed = layer_norm(hidden.astype(jnp.float32), norm_eps).astype(jnp.bfloat16)
    proj = jax.nn.silu(jnp.dot(normed, weight_in, preferred_element_type=jnp.float32)).astype(jnp.bfloat16)
    gate_part = proj[:, :width]
    value_part = proj[:, width:2 * width]
    query_part = proj[:, 2 * width:3 * width]
    key_part = proj[:, 3 * width:]
    places = jnp.arange(rows, dtype=jnp.int32)
    stream = lax.optimization_barrier(jnp.sum((places[:, None] >= bounds[None, :]).astype(jnp.int32), axis=1))
    live = places % TOK_DEV < valid_row[places // TOK_DEV]
    key_pad = jnp.concatenate([jnp.zeros((WINDOW, width), key_part.dtype), key_part], 0)
    value_pad = jnp.concatenate([jnp.zeros((WINDOW, width), value_part.dtype), value_part], 0)
    stream_pad = jnp.concatenate([jnp.zeros((WINDOW,), jnp.int32) - 1, stream], 0)
    live_pad = jnp.concatenate([jnp.zeros((WINDOW,), bool), live], 0)
    span = TOK_DEV + WINDOW
    score_scale = 1.0 / math.sqrt(HEAD_DIM)
    mix_scale = 1.0 / math.sqrt(WINDOW)

    def block(index):
        start = (index * TOK_DEV).astype(jnp.int32)
        query = lax.dynamic_slice_in_dim(query_part, start, TOK_DEV, 0).astype(jnp.float32)
        keys = lax.dynamic_slice_in_dim(key_pad, start, span, 0).astype(jnp.float32)
        values = lax.dynamic_slice_in_dim(value_pad, start, span, 0).astype(jnp.float32)
        query_stream = lax.dynamic_slice_in_dim(stream, start, TOK_DEV, 0)
        key_stream = lax.dynamic_slice_in_dim(stream_pad, start, span, 0)
        query_live = lax.dynamic_slice_in_dim(live, start, TOK_DEV, 0)
        key_live = lax.dynamic_slice_in_dim(live_pad, start, span, 0)
        query_pos = start + jnp.arange(TOK_DEV, dtype=jnp.int32)
        key_pos = start - WINDOW + jnp.arange(span, dtype=jnp.int32)
        allowed = query_live[:, None] & key_live[None, :] & (query_stream[:, None] == key_stream[None, :]) & (key_pos[None, :] <= query_pos[:, None]) & (query_pos[:, None] - key_pos[None, :] < WINDOW) & (key_pos[None, :] >= 0)
        scores = jnp.einsum('qhd,khd->hqk', query.reshape(TOK_DEV, HEADS, HEAD_DIM), keys.reshape(span, HEADS, HEAD_DIM))
        weights = jnp.where(allowed[None], jax.nn.silu(scores * score_scale) * mix_scale, 0.0).astype(jnp.bfloat16)
        mixed = jnp.einsum('hqk,khd->qhd', weights.astype(jnp.float32), values.reshape(span, HEADS, HEAD_DIM))
        return mixed.reshape(TOK_DEV, width)
    attended = lax.map(block, jnp.arange(rows // TOK_DEV, dtype=jnp.int32)).reshape(rows, width)
    gated = (layer_norm(attended, out_eps) * gate_part.astype(jnp.float32)).astype(jnp.bfloat16)
    return (hidden.astype(jnp.float32) + jnp.dot(gated, weight_out, preferred_element_type=jnp.float32)).astype(jnp.bfloat16)

def reference(inputs, w_in, w_out, lengths, valid):
    results = []
    current = [inputs[m] for m in range(MICRO)]
    for layer in range(LAYERS):
        outputs = []
        for m in range(MICRO):
            bounds = jnp.cumsum(lengths[m]).astype(jnp.int32)
            outputs.append(one_layer(current[m], w_in[layer], w_out[layer], bounds, valid[m]))
        results.append(jnp.stack(outputs, 0))
        current = outputs
    return jnp.stack(results, 0)
```

```python
import functools
import math

import jax
import jax.numpy as jnp
from jax import lax
from jax.experimental import pallas as pl
from jax.experimental.pallas import tpu as pltpu
from jax.sharding import PartitionSpec as P

HEAD_DIM = 128
WINDOW = 512
TILE = 128
ROW_TILE = 256

norm_eps = 1e-05
out_eps = 0.001

FAR = 1 << 30


def shifted(x, axis, by):
    size = lax.axis_size(axis)
    pairs = [(i, i + by) for i in range(size) if 0 <= i + by < size]
    return lax.ppermute(x, axis, pairs)


def normalise(values, epsilon):
    mean = jnp.mean(values, axis=-1, keepdims=True)
    centred = values - mean
    spread = jnp.mean(centred * centred, axis=-1, keepdims=True)
    return centred * lax.rsqrt(spread + epsilon)


def half_silu(half):
    return half + half * jnp.tanh(half)


def stream_floor(lengths, slot, base, rows):
    place = base + lax.broadcasted_iota(jnp.int32, (rows, TILE), 0)
    bound = jnp.int32(0)
    start = jnp.zeros((rows, TILE), jnp.int32)
    for k in range(lengths.shape[1]):
        bound = bound + lengths[slot, k]
        start = jnp.where(place >= bound, bound, start)
    return start - base


def own_kernel(spot, lengths, valid, x, w_in, gates, queries, mixed, keys, values, *, micro):
    tok = x.shape[1]
    branch = w_in.shape[1] // 4
    heads = branch // HEAD_DIM
    scale = 0.5 / math.sqrt(HEAD_DIM)
    block = spot[0]

    def one(m, _):
        slot = spot[1] + m
        for r in range(0, tok, ROW_TILE):
            rows = pl.ds(r, ROW_TILE)
            normed = normalise(x[m, rows, :].astype(jnp.float32), norm_eps).astype(jnp.bfloat16)
            for part in range(4):
                half = 0.5 * jnp.dot(
                    normed,
                    w_in[:, part * branch : (part + 1) * branch],
                    preferred_element_type=jnp.float32,
                )
                out = half_silu(half).astype(jnp.bfloat16)
                if part == 0:
                    gates[m, rows, :] = out
                elif part == 1:
                    values[rows, :] = out
                elif part == 2:
                    queries[m, rows, :] = out
                else:
                    keys[rows, :] = out
        floor = stream_floor(lengths, slot, block * tok, tok)
        count = valid[slot, block]
        for t in range(0, tok, TILE):
            span = t + TILE
            row = t + lax.broadcasted_iota(jnp.int32, (TILE, span), 0)
            col = lax.broadcasted_iota(jnp.int32, (TILE, span), 1)
            low = jnp.concatenate([floor[t : t + TILE]] * (span // TILE), 1)
            allowed = (col <= row) & (col >= low) & (row < count)
            for h in range(heads):
                lanes = slice(h * HEAD_DIM, (h + 1) * HEAD_DIM)
                half = scale * lax.dot_general(
                    queries[m, t : t + TILE, lanes],
                    keys[0:span, lanes],
                    (((1,), (1,)), ((), ())),
                    preferred_element_type=jnp.float32,
                )
                weights = jnp.where(allowed, half_silu(half), 0.0).astype(jnp.bfloat16)
                mixed[m, t : t + TILE, lanes] = jnp.dot(
                    weights, values[0:span, lanes], preferred_element_type=jnp.float32
                )
        return 0

    lax.fori_loop(0, micro, one, 0)


def far_kernel(
    spot, lengths, valid, before, x, w_in, w_out, gates, queries, mixed, *rest, offset
):
    out, keys, values = rest[-3:]
    tok = x.shape[1]
    branch = w_out.shape[0]
    heads = branch // HEAD_DIM
    scale = 0.5 / math.sqrt(HEAD_DIM)
    block = spot[0]
    slot = spot[1] + offset
    m = offset
    for r in range(0, tok, ROW_TILE):
        rows = pl.ds(r, ROW_TILE)
        normed = normalise(before[rows, :].astype(jnp.float32), norm_eps).astype(jnp.bfloat16)
        for part, kept in ((1, values), (3, keys)):
            half = 0.5 * jnp.dot(
                normed,
                w_in[:, part * branch : (part + 1) * branch],
                preferred_element_type=jnp.float32,
            )
            kept[rows, :] = half_silu(half).astype(jnp.bfloat16)
    floor = stream_floor(lengths, slot, block * tok, tok)
    count = valid[slot, block]
    count_before = valid[slot, jnp.maximum(block - 1, 0)]
    for t in range(tok - TILE, -1, -TILE):
        span = tok - t
        row = t + lax.broadcasted_iota(jnp.int32, (TILE, span), 0)
        col = t + lax.broadcasted_iota(jnp.int32, (TILE, span), 1)
        low = jnp.concatenate([floor[t : t + TILE]] * (span // TILE), 1) + tok
        allowed = (col > row) & (col >= low) & (col < count_before) & (row < count)
        parts = []
        for h in range(heads):
            lanes = slice(h * HEAD_DIM, (h + 1) * HEAD_DIM)
            half = scale * lax.dot_general(
                queries[m, t : t + TILE, lanes],
                keys[t:tok, lanes],
                (((1,), (1,)), ((), ())),
                preferred_element_type=jnp.float32,
            )
            weights = jnp.where(allowed, half_silu(half), 0.0).astype(jnp.bfloat16)
            parts.append(
                mixed[m, t : t + TILE, lanes]
                + jnp.dot(weights, values[t:tok, lanes], preferred_element_type=jnp.float32)
            )
        attended = normalise(jnp.concatenate(parts, 1), out_eps * WINDOW)
        gated = (attended * gates[m, t : t + TILE, :].astype(jnp.float32)).astype(jnp.bfloat16)
        out[0, 0, t : t + TILE, :] = (
            x[m, t : t + TILE, :].astype(jnp.float32)
            + jnp.dot(gated, w_out[...], preferred_element_type=jnp.float32)
        ).astype(jnp.bfloat16)


SMEM = pl.BlockSpec(memory_space=pltpu.SMEM)
VMEM = pl.BlockSpec(memory_space=pltpu.VMEM)
ANY = pl.BlockSpec(memory_space=pl.ANY)


def layer(x, w_in, w_out, lengths, valid, slot):
    micro, tok, width = x.shape
    branch = w_out.shape[0]
    spot = jnp.stack([lax.axis_index("seq").astype(jnp.int32), slot])
    arrived = [shifted(x[m], "seq", 1) for m in range(micro)]
    gates, queries, mixed = pl.pallas_call(
        functools.partial(own_kernel, micro=micro),
        out_shape=(
            jax.ShapeDtypeStruct((micro, tok, branch), jnp.bfloat16),
            jax.ShapeDtypeStruct((micro, tok, branch), jnp.bfloat16),
            jax.ShapeDtypeStruct((micro, tok, branch), jnp.float32),
        ),
        in_specs=[SMEM, SMEM, SMEM, VMEM, VMEM],
        out_specs=(VMEM, VMEM, VMEM),
        scratch_shapes=[
            pltpu.VMEM((tok, branch), jnp.bfloat16),
            pltpu.VMEM((tok, branch), jnp.bfloat16),
        ],
        compiler_params=pltpu.CompilerParams(vmem_limit_bytes=24 << 20),
        cost_estimate=pl.CostEstimate(
            flops=micro * tok * branch * (8 * width + 4 * tok),
            transcendentals=micro * tok * branch * 6,
            bytes_accessed=6 << 20,
        ),
        name="own",
    )(spot, lengths, valid, x, w_in)
    states = None
    for m in range(micro):
        operands = [spot, lengths, valid, arrived[m], x, w_in, w_out, gates, queries, mixed]
        specs = [SMEM] * 3 + [VMEM] * 7
        aliases = {}
        if states is not None:
            aliases = {len(operands): 0}
            operands.append(states)
            specs.append(ANY)
        states = pl.pallas_call(
            functools.partial(far_kernel, offset=m),
            out_shape=jax.ShapeDtypeStruct((1, micro, tok, width), jnp.bfloat16),
            grid=(1,),
            in_specs=specs,
            out_specs=pl.BlockSpec((1, 1, tok, width), lambda i, m=m: (0, m, 0, 0)),
            scratch_shapes=[
                pltpu.VMEM((tok, branch), jnp.bfloat16),
                pltpu.VMEM((tok, branch), jnp.bfloat16),
            ],
            input_output_aliases=aliases,
            compiler_params=pltpu.CompilerParams(vmem_limit_bytes=24 << 20),
            cost_estimate=pl.CostEstimate(
                flops=tok * branch * (6 * width + 4 * tok),
                transcendentals=tok * branch * 4,
                bytes_accessed=6 << 20,
            ),
            name="far",
        )(*operands)
    return states[0]


def shards(inputs, w_in, w_out, lengths, valid):
    micro, tok, width = inputs.shape
    sections = lax.axis_size("pipe")
    if sections == 1:
        return layer(inputs, w_in[0], w_out[0], lengths, valid, jnp.int32(0))[None]
    section = lax.axis_index("pipe")

    def tick(step, carry):
        incoming, states = carry
        slot = step - section
        active = (slot >= 0) & (slot < micro)
        index = jnp.clip(slot, 0, micro - 1)
        fresh = lax.dynamic_index_in_dim(inputs, index, 0, keepdims=False)
        x_rows = jnp.where(section == 0, fresh, incoming)
        result = layer(x_rows[None], w_in[0], w_out[0], lengths, valid, index)[0]
        updated = lax.dynamic_update_slice(
            states, result[None, None], (jnp.int32(0), index, jnp.int32(0), jnp.int32(0))
        )
        states = jnp.where(active, updated, states)
        return (shifted(result, "pipe", 1), states)

    start_states = jnp.zeros((1, micro, tok, width), jnp.bfloat16)
    start_rows = jnp.zeros((tok, width), jnp.bfloat16)
    _, states = lax.fori_loop(0, sections + micro - 1, tick, (start_rows, start_states))
    return states


def solution(mesh):
    in_specs = (P(None, "seq", None), P("pipe", None, None), P("pipe", None, None), P(), P())
    out_specs = P("pipe", None, "seq", None)
    return jax.shard_map(shards, mesh=mesh, in_specs=in_specs, out_specs=out_specs, check_vma=False)
```

```python
import functools
import math

import jax
import jax.numpy as jnp
from jax import lax
from jax.experimental import pallas as pl
from jax.experimental.pallas import tpu as pltpu
from jax.sharding import PartitionSpec as P

HEAD_DIM = 128
WINDOW = 512
BLOCK = 256
LATE = (3, 4)

norm_eps = 1e-05
out_eps = 0.001

FAR = 1 << 30


def shifted(x, axis, by):
    size = lax.axis_size(axis)
    pairs = [(i, i + by) for i in range(size) if 0 <= i + by < size]
    return lax.ppermute(x, axis, pairs)


def normalise(values, epsilon, factor=1.0):
    mean = jnp.mean(values, axis=-1, keepdims=True)
    centred = values - mean
    spread = jnp.mean(centred * centred, axis=-1, keepdims=True)
    return centred * (factor * lax.rsqrt(spread + epsilon))


def half_silu(half):
    return half + half * jnp.tanh(half)


def dot(a, b):
    return jnp.dot(a, b, preferred_element_type=jnp.float32)


def dot_rows(a, b):
    return lax.dot_general(a, b, (((1,), (1,)), ((), ())), preferred_element_type=jnp.float32)


def lanes(head):
    return slice(head * HEAD_DIM, (head + 1) * HEAD_DIM)


def wide(columns, width):
    return jnp.concatenate([columns] * (width // columns.shape[1]), 1)


def places(top, bottom, left, right):
    shape = (bottom - top, right - left)
    row = top + lax.broadcasted_iota(jnp.int32, shape, 0)
    col = left + lax.broadcasted_iota(jnp.int32, shape, 1)
    return row, col


def local_blocks(low, high):
    edges = [low, *[e for e in range(0, high, BLOCK) if e > low], high]
    return list(zip(edges[:-1], edges[1:]))


def rows_of(first, second, micro, tok, m, top, bottom):
    late = second.shape[0]
    if m < micro - 1:
        return first[m * tok + top : m * tok + bottom, :]
    if top >= late:
        return first[m * tok + top - late : m * tok + bottom - late, :]
    if bottom <= late:
        return second[top:bottom, :]
    return jnp.concatenate([second[top:late, :], first[m * tok : m * tok + bottom - late, :]], 0)


def cut_kernel(x, first, second, sems):
    micro, tok, _ = x.shape
    late = second.shape[0]
    last = micro - 1
    copies = [
        (x.at[m], first.at[pl.ds(m * tok, tok)]) for m in range(last)
    ] + [
        (x.at[last, pl.ds(late, tok - late)], first.at[pl.ds(last * tok, tok - late)]),
        (x.at[last, pl.ds(0, late)], second),
    ]
    copies = [pltpu.make_async_copy(a, b, sems.at[i]) for i, (a, b) in enumerate(copies)]
    for copy in copies:
        copy.start()
    for copy in copies:
        copy.wait()


def own_kernel(
    slot, first, second, w_in, lengths, valid,
    gates, queries, mixed, w_kv, floors, counts,
    w_q, w_u, normed, keys, values, spans, alive, sems,
    *, micro, tok,
):
    branch = w_q.shape[1]
    heads = branch // HEAD_DIM
    scale = 0.5 / math.sqrt(HEAD_DIM)
    block = lax.axis_index("seq")
    parts = {
        1: (w_kv.at[:, pl.ds(0, branch)], values),
        3: (w_kv.at[:, pl.ds(branch, branch)], keys),
        2: (w_q, queries),
        0: (w_u, gates),
    }
    small = [
        pltpu.make_async_copy(lengths, spans, sems.at[4]),
        pltpu.make_async_copy(valid, alive, sems.at[5]),
    ]
    loads = {
        part: pltpu.make_async_copy(w_in.at[:, pl.ds(part * branch, branch)], there, sems.at[part])
        for part, (there, _) in parts.items()
    }
    for copy in [*loads.values(), *small]:
        copy.start()
    for m in range(micro):
        for top in range(0, tok, 128):
            rows = rows_of(first, second, micro, tok, m, top, top + 128).astype(jnp.float32)
            normed[m * tok + top : m * tok + top + 128, :] = normalise(rows, norm_eps, 0.5).astype(
                jnp.bfloat16
            )
    for part, (weight, kept) in parts.items():
        loads[part].wait()
        for m in range(micro):
            out = half_silu(dot(normed[m * tok : (m + 1) * tok, :], weight[...]))
            kept[m] = (out * scale if part == 2 else out).astype(jnp.bfloat16)
    for copy in small:
        copy.wait()
    for m in range(micro):
        row = lax.broadcasted_iota(jnp.int32, (tok, 128), 0)
        place = block * tok + row
        bound = jnp.int32(0)
        start = jnp.zeros((tok, 128), jnp.int32)
        for k in range(spans.shape[1]):
            bound = bound + spans[slot + m, k]
            start = jnp.where(place >= bound, bound, start)
        floors[m] = jnp.where(row < alive[slot + m, block], start - block * tok, FAR)
        counts[m] = jnp.full((8, 128), alive[slot + m, jnp.maximum(block - 1, 0)], jnp.int32)
    pending = []

    def finish(m, head, pieces):
        total = {}
        for (left, right), weights in pieces:
            product = dot(weights, values[m, left:right, lanes(head)])
            for top in range(left, tok, BLOCK):
                piece = product[top - left : top - left + BLOCK]
                total[top] = total[top] + piece if top in total else piece
        mixed[m, :, lanes(head)] = jnp.concatenate([total[t] for t in sorted(total)], 0)

    for m in range(micro):
        masks = {}
        for left, right in local_blocks(0, tok):
            row, col = places(left, tok, left, right)
            masks[left] = (col <= row) & (col >= wide(floors[m, left:tok], right - left))
        for head in range(heads):
            pieces = []
            for left, right in local_blocks(0, tok):
                half = dot_rows(queries[m, left:tok, lanes(head)], keys[m, left:right, lanes(head)])
                weights = jnp.where(masks[left], half_silu(half), 0.0).astype(jnp.bfloat16)
                pieces.append(((left, right), weights))
            pending.append((m, head, pieces))
            if len(pending) > 1:
                finish(*pending.pop(0))
    finish(*pending.pop(0))


def far_rows(before, w_kv, keys, values):
    branch = keys.shape[1]
    rows = before.shape[0]
    for top in range(0, rows, BLOCK):
        bottom = min(top + BLOCK, rows)
        normed = normalise(before[top:bottom, :].astype(jnp.float32), norm_eps, 0.5)
        normed = normed.astype(jnp.bfloat16)
        values[top:bottom, :] = half_silu(dot(normed, w_kv[:, :branch])).astype(jnp.bfloat16)
        keys[top:bottom, :] = half_silu(dot(normed, w_kv[:, branch:])).astype(jnp.bfloat16)


def far_sums(low, high, offset, queries, mixed, floors, counts, keys, values, m, tok):
    blocks = local_blocks(low, high)[::-1]
    edges = sorted({0, *[e for b in blocks for e in b if e > 0]})
    masks = {}
    for left, right in blocks:
        row, col = places(0, right, left, right)
        reach = wide(jnp.concatenate([counts[m]] * (right // 8), 0), right - left)
        earliest = wide(floors[m, 0:right], right - left) + tok
        masks[left] = (col > row) & (col >= earliest) & (col < reach)
    sums = []
    pending = []

    def finish(head, pieces):
        total = {top: mixed[m, top:bottom, lanes(head)] for top, bottom in zip(edges, edges[1:])}
        for (left, right), weights in pieces:
            product = dot(weights, values[offset + left : offset + right, lanes(head)])
            for top, bottom in zip(edges, edges[1:]):
                if bottom <= right:
                    total[top] = total[top] + product[top:bottom]
        sums.append(jnp.concatenate([total[t] for t in sorted(total)], 0))

    for head in range(queries.shape[2] // HEAD_DIM):
        pieces = []
        for left, right in blocks:
            half = dot_rows(
                queries[m, 0:right, lanes(head)],
                keys[offset + left : offset + right, lanes(head)],
            )
            weights = jnp.where(masks[left], half_silu(half), 0.0).astype(jnp.bfloat16)
            pieces.append(((left, right), weights))
        pending.append((head, pieces))
        if len(pending) > 1:
            finish(*pending.pop(0))
    finish(*pending.pop(0))
    return sums


def close(sums, top, bottom, x_rows, w_out, gates, m, done, out, sems, number):
    copies = []
    for low in range(top, bottom, BLOCK):
        high = min(low + BLOCK, bottom)
        attended = jnp.concatenate([s[low:high] for s in sums], 1)
        attended = normalise(attended, out_eps * WINDOW)
        gated = (attended * gates[m, low:high, :].astype(jnp.float32)).astype(jnp.bfloat16)
        result = x_rows(m, low, high).astype(jnp.float32) + dot(gated, w_out[...])
        done[m, low:high, :] = result.astype(jnp.bfloat16)
        copies.append(
            pltpu.make_async_copy(
                done.at[m, pl.ds(low, high - low)],
                out.at[0, m, pl.ds(low, high - low)],
                sems.at[number + len(copies)],
            )
        )
        copies[-1].start()
    return copies


def far_first_kernel(
    before, first, second, w_kv, w_out, gates, queries, mixed, floors, counts,
    out, rest, keys, values, done, sems, *, micro, tok,
):
    late = second.shape[0]
    last = micro - 1
    x_rows = functools.partial(rows_of, first, second, micro, tok)
    far_rows(before, w_kv, keys, values)
    copies = []
    for m in range(last):
        sums = far_sums(0, tok, m * tok, queries, mixed, floors, counts, keys, values, m, tok)
        copies += close(sums, 0, tok, x_rows, w_out, gates, m, done, out, sems, len(copies))
    sums = far_sums(
        late, tok, last * tok - late, queries, mixed, floors, counts, keys, values, last, tok
    )
    for head, total in enumerate(sums):
        rest[0, :, lanes(head)] = total[:late]
    copies += close(sums, late, tok, x_rows, w_out, gates, last, done, out, sems, len(copies))
    for copy in copies:
        copy.wait()


def far_second_kernel(
    before, second, w_kv, w_out, gates, queries, rest, floors, counts, _,
    out, keys, values, done, sems, *, tok,
):
    late = second.shape[0]
    last = gates.shape[0] - 1
    far_rows(before, w_kv, keys, values)

    class Last:
        def __getitem__(self, index):
            return rest[(0, *index[1:])]

    sums = far_sums(0, late, 0, queries, Last(), floors, counts, keys, values, last, tok)
    for copy in close(
        sums, 0, late, lambda m, top, bottom: second[top:bottom, :],
        w_out, gates, last, done, out, sems, 0,
    ):
        copy.wait()


VMEM = pl.BlockSpec(memory_space=pltpu.VMEM)
SMEM = pl.BlockSpec(memory_space=pltpu.SMEM)
HBM = pl.BlockSpec(memory_space=pltpu.HBM)


def layer(x, w_in, w_out, lengths, valid, slot):
    micro, tok, width = x.shape
    branch = w_out.shape[0]
    late = tok * LATE[0] // LATE[1]
    early = micro * tok - late
    bf16, f32, i32 = jnp.bfloat16, jnp.float32, jnp.int32
    shape = jax.ShapeDtypeStruct
    params = pltpu.CompilerParams(vmem_limit_bytes=24 << 20)

    def cost(rows, flops, tanhs):
        return pl.CostEstimate(
            flops=rows * flops, transcendentals=rows * tanhs, bytes_accessed=4 << 20
        )

    first, second = pl.pallas_call(
        cut_kernel,
        out_shape=(shape((early, width), bf16), shape((late, width), bf16)),
        in_specs=[HBM],
        out_specs=(VMEM, VMEM),
        scratch_shapes=[pltpu.SemaphoreType.DMA((micro + 1,))],
        compiler_params=params,
        name="cut",
    )(x)
    first_come = shifted(first, "seq", 1)
    second_come = shifted(second, "seq", 1)

    gates, queries, mixed, w_kv, floors, counts = pl.pallas_call(
        functools.partial(own_kernel, slot, micro=micro, tok=tok)
        if isinstance(slot, int)
        else functools.partial(own_kernel_at, micro=micro, tok=tok),
        out_shape=(
            shape((micro, tok, branch), bf16),
            shape((micro, tok, branch), bf16),
            shape((micro, tok, branch), f32),
            shape((width, 2 * branch), bf16),
            shape((micro, tok, 128), i32),
            shape((micro, 8, 128), i32),
        ),
        in_specs=([] if isinstance(slot, int) else [SMEM]) + [VMEM, VMEM, HBM, HBM, HBM],
        out_specs=(VMEM,) * 6,
        scratch_shapes=[
            pltpu.VMEM((width, branch), bf16),
            pltpu.VMEM((width, branch), bf16),
            pltpu.VMEM((micro * tok, width), bf16),
            pltpu.VMEM((micro, tok, branch), bf16),
            pltpu.VMEM((micro, tok, branch), bf16),
            pltpu.SMEM(lengths.shape, i32),
            pltpu.SMEM(valid.shape, i32),
            pltpu.SemaphoreType.DMA((6,)),
        ],
        compiler_params=params,
        cost_estimate=cost(micro * tok, branch * (8 * width + 4 * tok), branch * 6),
        name="own",
    )(*([] if isinstance(slot, int) else [slot[None]]), first, second, w_in, lengths, valid)
    states, rest = pl.pallas_call(
        functools.partial(far_first_kernel, micro=micro, tok=tok),
        out_shape=(shape((1, micro, tok, width), bf16), shape((1, late, branch), f32)),
        in_specs=[VMEM] * 10,
        out_specs=(HBM, VMEM),
        scratch_shapes=[
            pltpu.VMEM((early, branch), bf16),
            pltpu.VMEM((early, branch), bf16),
            pltpu.VMEM((micro, tok, width), bf16),
            pltpu.SemaphoreType.DMA((micro * (tok // BLOCK + 1),)),
        ],
        compiler_params=params,
        cost_estimate=cost(early, branch * (6 * width + 4 * tok), branch * 4),
        name="far_first",
    )(first_come, first, second, w_kv, w_out, gates, queries, mixed, floors, counts)
    return pl.pallas_call(
        functools.partial(far_second_kernel, tok=tok),
        out_shape=shape((1, micro, tok, width), bf16),
        in_specs=[VMEM] * 9 + [HBM],
        out_specs=HBM,
        scratch_shapes=[
            pltpu.VMEM((late, branch), bf16),
            pltpu.VMEM((late, branch), bf16),
            pltpu.VMEM((micro, tok, width), bf16),
            pltpu.SemaphoreType.DMA((late // BLOCK + 1,)),
        ],
        input_output_aliases={9: 0},
        compiler_params=params,
        cost_estimate=cost(late, branch * (6 * width + 4 * tok), branch * 4),
        name="far_second",
    )(second_come, second, w_kv, w_out, gates, queries, rest, floors, counts, states)[0]


def own_kernel_at(slot, *refs, micro, tok):
    own_kernel(slot[0], *refs, micro=micro, tok=tok)


def shards(inputs, w_in, w_out, lengths, valid):
    micro, tok, width = inputs.shape
    sections = lax.axis_size("pipe")
    if sections == 1:
        return layer(inputs, w_in[0], w_out[0], lengths, valid, 0)[None]
    section = lax.axis_index("pipe")

    def tick(step, carry):
        incoming, states = carry
        slot = step - section
        active = (slot >= 0) & (slot < micro)
        index = jnp.clip(slot, 0, micro - 1)
        fresh = lax.dynamic_index_in_dim(inputs, index, 0, keepdims=False)
        x_rows = jnp.where(section == 0, fresh, incoming)
        result = layer(x_rows[None], w_in[0], w_out[0], lengths, valid, index)[0]
        updated = lax.dynamic_update_slice(
            states, result[None, None], (jnp.int32(0), index, jnp.int32(0), jnp.int32(0))
        )
        states = jnp.where(active, updated, states)
        return (shifted(result, "pipe", 1), states)

    start_states = jnp.zeros((1, micro, tok, width), jnp.bfloat16)
    start_rows = jnp.zeros((tok, width), jnp.bfloat16)
    _, states = lax.fori_loop(0, sections + micro - 1, tick, (start_rows, start_states))
    return states


def solution(mesh):
    in_specs = (P(None, "seq", None), P("pipe", None, None), P("pipe", None, None), P(), P())
    out_specs = P("pipe", None, "seq", None)
    return jax.shard_map(shards, mesh=mesh, in_specs=in_specs, out_specs=out_specs, check_vma=False)
```

```python
import functools
import math

import jax
import jax.numpy as jnp
from jax import lax
from jax.experimental import pallas as pl
from jax.experimental.pallas import tpu as pltpu
from jax.sharding import PartitionSpec as P

HEAD_DIM = 128
WINDOW = 512
BLOCK = 256
LATE = (3, 4)

norm_eps = 1e-05
out_eps = 0.001

FAR = 1 << 30


def shifted(x, axis, by):
    size = lax.axis_size(axis)
    pairs = [(i, i + by) for i in range(size) if 0 <= i + by < size]
    return lax.ppermute(x, axis, pairs)


def normalise(values, epsilon, factor=1.0):
    mean = jnp.mean(values, axis=-1, keepdims=True)
    centred = values - mean
    spread = jnp.mean(centred * centred, axis=-1, keepdims=True)
    return centred * (factor * lax.rsqrt(spread + epsilon))


def half_silu(half):
    return half + half * jnp.tanh(half)


def dot(a, b):
    return jnp.dot(a, b, preferred_element_type=jnp.float32)


def dot_rows(a, b):
    return lax.dot_general(a, b, (((1,), (1,)), ((), ())), preferred_element_type=jnp.float32)


def lanes(head):
    return slice(head * HEAD_DIM, (head + 1) * HEAD_DIM)


def wide(columns, width):
    return jnp.concatenate([columns] * (width // columns.shape[1]), 1)


def places(top, bottom, left, right):
    shape = (bottom - top, right - left)
    row = top + lax.broadcasted_iota(jnp.int32, shape, 0)
    col = left + lax.broadcasted_iota(jnp.int32, shape, 1)
    return row, col


def local_blocks(low, high):
    edges = [low, *[e for e in range(0, high, BLOCK) if e > low], high]
    return list(zip(edges[:-1], edges[1:]))


def rows_of(first, second, micro, tok, m, top, bottom):
    late = second.shape[0]
    if m < micro - 1:
        return first[m * tok + top : m * tok + bottom, :]
    if top >= late:
        return first[m * tok + top - late : m * tok + bottom - late, :]
    if bottom <= late:
        return second[top:bottom, :]
    return jnp.concatenate([second[top:late, :], first[m * tok : m * tok + bottom - late, :]], 0)


def cut_kernel(x, first, second, sems):
    micro, tok, _ = x.shape
    late = second.shape[0]
    last = micro - 1
    copies = [
        (x.at[m], first.at[pl.ds(m * tok, tok)]) for m in range(last)
    ] + [
        (x.at[last, pl.ds(late, tok - late)], first.at[pl.ds(last * tok, tok - late)]),
        (x.at[last, pl.ds(0, late)], second),
    ]
    copies = [pltpu.make_async_copy(a, b, sems.at[i]) for i, (a, b) in enumerate(copies)]
    for copy in copies:
        copy.start()
    for copy in copies:
        copy.wait()


def own_kernel(
    slot, first, second, w_in, lengths, valid,
    gates, queries, mixed, w_kv, floors, counts,
    w_q, w_u, normed, keys, values, spans, alive, sems,
    *, micro, tok,
):
    branch = w_q.shape[1]
    heads = branch // HEAD_DIM
    scale = 0.5 / math.sqrt(HEAD_DIM)
    block = lax.axis_index("seq")
    parts = {
        1: (w_kv.at[:, pl.ds(0, branch)], values),
        3: (w_kv.at[:, pl.ds(branch, branch)], keys),
        2: (w_q, queries),
        0: (w_u, gates),
    }
    small = [
        pltpu.make_async_copy(lengths, spans, sems.at[4]),
        pltpu.make_async_copy(valid, alive, sems.at[5]),
    ]
    loads = {
        part: pltpu.make_async_copy(w_in.at[:, pl.ds(part * branch, branch)], there, sems.at[part])
        for part, (there, _) in parts.items()
    }
    for copy in [*loads.values(), *small]:
        copy.start()
    for m in range(micro):
        for top in range(0, tok, 128):
            rows = rows_of(first, second, micro, tok, m, top, top + 128).astype(jnp.float32)
            normed[m * tok + top : m * tok + top + 128, :] = normalise(rows, norm_eps, 0.5).astype(
                jnp.bfloat16
            )
    for part, (weight, kept) in parts.items():
        loads[part].wait()
        for m in range(micro):
            out = half_silu(dot(normed[m * tok : (m + 1) * tok, :], weight[...]))
            kept[m] = (out * scale if part == 2 else out).astype(jnp.bfloat16)
    for copy in small:
        copy.wait()
    for m in range(micro):
        row = lax.broadcasted_iota(jnp.int32, (tok, 128), 0)
        place = block * tok + row
        bound = jnp.int32(0)
        start = jnp.zeros((tok, 128), jnp.int32)
        for k in range(spans.shape[1]):
            bound = bound + spans[slot + m, k]
            start = jnp.where(place >= bound, bound, start)
        floors[m] = jnp.where(row < alive[slot + m, block], start - block * tok, FAR)
        counts[m] = jnp.full((8, 128), alive[slot + m, jnp.maximum(block - 1, 0)], jnp.int32)
    pending = []

    def finish(m, head, pieces):
        total = {}
        for (left, right), weights in pieces:
            product = dot(weights, values[m, left:right, lanes(head)])
            for top in range(left, tok, BLOCK):
                piece = product[top - left : top - left + BLOCK]
                total[top] = total[top] + piece if top in total else piece
        mixed[m, :, lanes(head)] = jnp.concatenate([total[t] for t in sorted(total)], 0)

    for m in range(micro):
        masks = {}
        for left, right in local_blocks(0, tok):
            row, col = places(left, tok, left, right)
            masks[left] = (col <= row) & (col >= wide(floors[m, left:tok], right - left))
        for head in range(heads):
            pieces = []
            for left, right in local_blocks(0, tok):
                half = dot_rows(queries[m, left:tok, lanes(head)], keys[m, left:right, lanes(head)])
                weights = jnp.where(masks[left], half_silu(half), 0.0).astype(jnp.bfloat16)
                pieces.append(((left, right), weights))
            pending.append((m, head, pieces))
            if len(pending) > 1:
                finish(*pending.pop(0))
    finish(*pending.pop(0))


def far_rows(before, w_kv, keys, values):
    branch = keys.shape[1]
    rows = before.shape[0]
    for top in range(0, rows, BLOCK):
        bottom = min(top + BLOCK, rows)
        normed = normalise(before[top:bottom, :].astype(jnp.float32), norm_eps, 0.5)
        normed = normed.astype(jnp.bfloat16)
        values[top:bottom, :] = half_silu(dot(normed, w_kv[:, :branch])).astype(jnp.bfloat16)
        keys[top:bottom, :] = half_silu(dot(normed, w_kv[:, branch:])).astype(jnp.bfloat16)


def far_sums(low, high, offset, queries, mixed, floors, counts, keys, values, m, tok):
    blocks = local_blocks(low, high)[::-1]
    edges = sorted({0, *[e for b in blocks for e in b if e > 0]})
    masks = {}
    for left, right in blocks:
        row, col = places(0, right, left, right)
        reach = wide(jnp.concatenate([counts[m]] * (right // 8), 0), right - left)
        earliest = wide(floors[m, 0:right], right - left) + tok
        masks[left] = (col > row) & (col >= earliest) & (col < reach)
    sums = []
    pending = []

    def finish(head, pieces):
        total = {top: mixed[m, top:bottom, lanes(head)] for top, bottom in zip(edges, edges[1:])}
        for (left, right), weights in pieces:
            product = dot(weights, values[offset + left : offset + right, lanes(head)])
            for top, bottom in zip(edges, edges[1:]):
                if bottom <= right:
                    total[top] = total[top] + product[top:bottom]
        sums.append(jnp.concatenate([total[t] for t in sorted(total)], 0))

    for head in range(queries.shape[2] // HEAD_DIM):
        pieces = []
        for left, right in blocks:
            half = dot_rows(
                queries[m, 0:right, lanes(head)],
                keys[offset + left : offset + right, lanes(head)],
            )
            weights = jnp.where(masks[left], half_silu(half), 0.0).astype(jnp.bfloat16)
            pieces.append(((left, right), weights))
        pending.append((head, pieces))
        if len(pending) > 1:
            finish(*pending.pop(0))
    finish(*pending.pop(0))
    return sums


def close(sums, top, bottom, x_rows, w_out, gates, m, done, out, sems, number):
    copies = []
    for low in range(top, bottom, BLOCK):
        high = min(low + BLOCK, bottom)
        attended = jnp.concatenate([s[low:high] for s in sums], 1)
        attended = normalise(attended, out_eps * WINDOW)
        gated = (attended * gates[m, low:high, :].astype(jnp.float32)).astype(jnp.bfloat16)
        result = x_rows(m, low, high).astype(jnp.float32) + dot(gated, w_out[...])
        done[m, low:high, :] = result.astype(jnp.bfloat16)
        copies.append(
            pltpu.make_async_copy(
                done.at[m, pl.ds(low, high - low)],
                out.at[0, m, pl.ds(low, high - low)],
                sems.at[number + len(copies)],
            )
        )
        copies[-1].start()
    return copies


def far_first_kernel(
    before, first, second, w_kv, w_out, gates, queries, mixed, floors, counts,
    out, rest, keys, values, done, sems, *, micro, tok,
):
    late = second.shape[0]
    last = micro - 1
    x_rows = functools.partial(rows_of, first, second, micro, tok)
    far_rows(before, w_kv, keys, values)
    copies = []
    for m in range(last):
        sums = far_sums(0, tok, m * tok, queries, mixed, floors, counts, keys, values, m, tok)
        copies += close(sums, 0, tok, x_rows, w_out, gates, m, done, out, sems, len(copies))
    sums = far_sums(
        late, tok, last * tok - late, queries, mixed, floors, counts, keys, values, last, tok
    )
    for head, total in enumerate(sums):
        rest[0, :, lanes(head)] = total[:late]
    copies += close(sums, late, tok, x_rows, w_out, gates, last, done, out, sems, len(copies))
    for copy in copies:
        copy.wait()


def far_second_kernel(
    before, second, w_kv, w_out, gates, queries, rest, floors, counts, _,
    out, keys, values, done, sems, *, tok,
):
    late = second.shape[0]
    last = gates.shape[0] - 1
    far_rows(before, w_kv, keys, values)

    class Last:
        def __getitem__(self, index):
            return rest[(0, *index[1:])]

    sums = far_sums(0, late, 0, queries, Last(), floors, counts, keys, values, last, tok)
    for copy in close(
        sums, 0, late, lambda m, top, bottom: second[top:bottom, :],
        w_out, gates, last, done, out, sems, 0,
    ):
        copy.wait()


VMEM = pl.BlockSpec(memory_space=pltpu.VMEM)
SMEM = pl.BlockSpec(memory_space=pltpu.SMEM)
HBM = pl.BlockSpec(memory_space=pltpu.HBM)


def kept_in_hbm(x):
    return pltpu.with_memory_space_constraint(x, pltpu.HBM)


def layer(x, w_in, w_out, lengths, valid, slot):
    micro, tok, width = x.shape
    branch = w_out.shape[0]
    late = tok * LATE[0] // LATE[1]
    early = micro * tok - late
    bf16, f32, i32 = jnp.bfloat16, jnp.float32, jnp.int32
    shape = jax.ShapeDtypeStruct
    params = pltpu.CompilerParams(vmem_limit_bytes=24 << 20)

    def cost(rows, flops, tanhs):
        return pl.CostEstimate(
            flops=rows * flops, transcendentals=rows * tanhs, bytes_accessed=4 << 20
        )

    first, second = pl.pallas_call(
        cut_kernel,
        out_shape=(shape((early, width), bf16), shape((late, width), bf16)),
        in_specs=[HBM],
        out_specs=(VMEM, VMEM),
        scratch_shapes=[pltpu.SemaphoreType.DMA((micro + 1,))],
        compiler_params=params,
        name="cut",
    )(kept_in_hbm(x))
    first_come = shifted(first, "seq", 1)
    second_come = shifted(second, "seq", 1)

    gates, queries, mixed, w_kv, floors, counts = pl.pallas_call(
        functools.partial(own_kernel, slot, micro=micro, tok=tok)
        if isinstance(slot, int)
        else functools.partial(own_kernel_at, micro=micro, tok=tok),
        out_shape=(
            shape((micro, tok, branch), bf16),
            shape((micro, tok, branch), bf16),
            shape((micro, tok, branch), f32),
            shape((width, 2 * branch), bf16),
            shape((micro, tok, 128), i32),
            shape((micro, 8, 128), i32),
        ),
        in_specs=([] if isinstance(slot, int) else [SMEM]) + [VMEM, VMEM, HBM, HBM, HBM],
        out_specs=(VMEM,) * 6,
        scratch_shapes=[
            pltpu.VMEM((width, branch), bf16),
            pltpu.VMEM((width, branch), bf16),
            pltpu.VMEM((micro * tok, width), bf16),
            pltpu.VMEM((micro, tok, branch), bf16),
            pltpu.VMEM((micro, tok, branch), bf16),
            pltpu.SMEM(lengths.shape, i32),
            pltpu.SMEM(valid.shape, i32),
            pltpu.SemaphoreType.DMA((6,)),
        ],
        compiler_params=params,
        cost_estimate=cost(micro * tok, branch * (8 * width + 4 * tok), branch * 6),
        name="own",
    )(*([] if isinstance(slot, int) else [slot[None]]), first, second, *map(kept_in_hbm, (w_in, lengths, valid)))
    states, rest = pl.pallas_call(
        functools.partial(far_first_kernel, micro=micro, tok=tok),
        out_shape=(shape((1, micro, tok, width), bf16), shape((1, late, branch), f32)),
        in_specs=[VMEM] * 10,
        out_specs=(HBM, VMEM),
        scratch_shapes=[
            pltpu.VMEM((early, branch), bf16),
            pltpu.VMEM((early, branch), bf16),
            pltpu.VMEM((micro, tok, width), bf16),
            pltpu.SemaphoreType.DMA((micro * (tok // BLOCK + 1),)),
        ],
        compiler_params=params,
        cost_estimate=cost(early, branch * (6 * width + 4 * tok), branch * 4),
        name="far_first",
    )(first_come, first, second, w_kv, w_out, gates, queries, mixed, floors, counts)
    return pl.pallas_call(
        functools.partial(far_second_kernel, tok=tok),
        out_shape=shape((1, micro, tok, width), bf16),
        in_specs=[VMEM] * 9 + [HBM],
        out_specs=HBM,
        scratch_shapes=[
            pltpu.VMEM((late, branch), bf16),
            pltpu.VMEM((late, branch), bf16),
            pltpu.VMEM((micro, tok, width), bf16),
            pltpu.SemaphoreType.DMA((late // BLOCK + 1,)),
        ],
        input_output_aliases={9: 0},
        compiler_params=params,
        cost_estimate=cost(late, branch * (6 * width + 4 * tok), branch * 4),
        name="far_second",
    )(second_come, second, w_kv, w_out, gates, queries, rest, floors, counts, states)[0]


def own_kernel_at(slot, *refs, micro, tok):
    own_kernel(slot[0], *refs, micro=micro, tok=tok)


def shards(inputs, w_in, w_out, lengths, valid):
    micro, tok, width = inputs.shape
    sections = lax.axis_size("pipe")
    if sections == 1:
        return layer(inputs, w_in[0], w_out[0], lengths, valid, 0)[None]
    section = lax.axis_index("pipe")

    def tick(step, carry):
        incoming, states = carry
        slot = step - section
        active = (slot >= 0) & (slot < micro)
        index = jnp.clip(slot, 0, micro - 1)
        fresh = lax.dynamic_index_in_dim(inputs, index, 0, keepdims=False)
        x_rows = jnp.where(section == 0, fresh, incoming)
        result = layer(x_rows[None], w_in[0], w_out[0], lengths, valid, index)[0]
        updated = lax.dynamic_update_slice(
            states, result[None, None], (jnp.int32(0), index, jnp.int32(0), jnp.int32(0))
        )
        states = jnp.where(active, updated, states)
        return (shifted(result, "pipe", 1), states)

    start_states = jnp.zeros((1, micro, tok, width), jnp.bfloat16)
    start_rows = jnp.zeros((tok, width), jnp.bfloat16)
    _, states = lax.fori_loop(0, sections + micro - 1, tick, (start_rows, start_states))
    return states


def solution(mesh):
    in_specs = (P(None, "seq", None), P("pipe", None, None), P("pipe", None, None), P(), P())
    out_specs = P("pipe", None, "seq", None)
    return jax.shard_map(shards, mesh=mesh, in_specs=in_specs, out_specs=out_specs, check_vma=False)
```

```python
import functools
import math

import jax
import jax.numpy as jnp
from jax import lax
from jax.experimental import pallas as pl
from jax.experimental.pallas import tpu as pltpu
from jax.sharding import PartitionSpec as P

HEAD_DIM = 128
WINDOW = 512
BLOCK = 256
LATE_OTHER = 4
LATE_LAST = 2

norm_eps = 1e-05
out_eps = 0.001

FAR = 1 << 30


def shifted(x, axis, by):
    size = lax.axis_size(axis)
    pairs = [(i, i + by) for i in range(size) if 0 <= i + by < size]
    return lax.ppermute(x, axis, pairs)


def normalise(values, epsilon, factor=1.0):
    mean = jnp.mean(values, axis=-1, keepdims=True)
    centred = values - mean
    spread = jnp.mean(centred * centred, axis=-1, keepdims=True)
    return centred * (factor * lax.rsqrt(spread + epsilon))


def half_silu(half):
    return half + half * jnp.tanh(half)


def dot(a, b):
    return jnp.dot(a, b, preferred_element_type=jnp.float32)


def dot_rows(a, b):
    return lax.dot_general(a, b, (((1,), (1,)), ((), ())), preferred_element_type=jnp.float32)


def lanes(head):
    return slice(head * HEAD_DIM, (head + 1) * HEAD_DIM)


def wide(columns, width):
    return jnp.concatenate([columns] * (width // columns.shape[1]), 1)


def places(top, bottom, left, right):
    shape = (bottom - top, right - left)
    row = top + lax.broadcasted_iota(jnp.int32, shape, 0)
    col = left + lax.broadcasted_iota(jnp.int32, shape, 1)
    return row, col


def local_blocks(low, high):
    edges = [low, *[e for e in range(0, high, BLOCK) if e > low], high]
    return list(zip(edges[:-1], edges[1:]))


class Cut:
    def __init__(self, micro, tok):
        self.micro, self.tok = micro, tok
        self.late = [tok // LATE_OTHER] * (micro - 1) + [tok // LATE_LAST]
        self.second_at = [sum(self.late[:m]) for m in range(micro)]
        self.first_at = [m * tok - sum(self.late[:m]) for m in range(micro)]
        self.second_rows = sum(self.late)
        self.first_rows = micro * tok - self.second_rows

    def rows(self, first, second, m, top, bottom):
        late = self.late[m]
        early = self.first_at[m] - late
        if top >= late:
            return first[early + top : early + bottom, :]
        low = self.second_at[m]
        if bottom <= late:
            return second[low + top : low + bottom, :]
        parts = [second[low + top : low + late, :], first[early + late : early + bottom, :]]
        return jnp.concatenate(parts, 0)


def cut_kernel(x, first, sems, *, cut):
    copies = []
    for m in range(cut.micro):
        rows = cut.tok - cut.late[m]
        source = x.at[m, pl.ds(cut.late[m], rows)]
        target = first.at[pl.ds(cut.first_at[m], rows)]
        copies.append(pltpu.make_async_copy(source, target, sems.at[m]))
    for copy in copies:
        copy.start()
    for copy in copies:
        copy.wait()


def stream_floors(spans, slot, block, live, tok):
    row = lax.broadcasted_iota(jnp.int32, (8, tok), 1)
    bound = jnp.int32(0)
    start = jnp.zeros((8, tok), jnp.int32)
    for k in range(spans.shape[1]):
        bound = bound + spans[slot, k]
        start = jnp.where(block * tok + row >= bound, bound, start)
    start = jnp.where(row < live, start - block * tok, FAR)
    return jnp.transpose(jnp.concatenate([start] * 16, 0))


def project_kernel(
    slot, first, x, w_in, lengths, valid,
    second, second_normed, gates, queries, keys, values, w_kv, own_floors, floors, counts,
    w_q, w_u, normed, spans, alive, sems,
    *, cut,
):
    micro, tok = cut.micro, cut.tok
    branch = w_q.shape[1]
    scale = 0.5 / math.sqrt(HEAD_DIM)
    block = lax.axis_index("seq")
    parts = {
        1: (w_kv.at[:, pl.ds(0, branch)], values),
        3: (w_kv.at[:, pl.ds(branch, branch)], keys),
        2: (w_q, queries),
        0: (w_u, gates),
    }
    small = [
        pltpu.make_async_copy(lengths, spans, sems.at[4]),
        pltpu.make_async_copy(valid, alive, sems.at[5]),
    ]
    seconds = [
        pltpu.make_async_copy(
            x.at[m, pl.ds(0, cut.late[m])],
            second.at[pl.ds(cut.second_at[m], cut.late[m])],
            sems.at[6 + m],
        )
        for m in range(micro)
    ]
    loads = {
        part: pltpu.make_async_copy(w_in.at[:, pl.ds(part * branch, branch)], there, sems.at[part])
        for part, (there, _) in parts.items()
    }
    queue = [*seconds, *small, *loads.values()]
    for copy in queue[:-3]:
        copy.start()

    def norm_rows(rows):
        return normalise(rows.astype(jnp.float32), norm_eps, 0.5).astype(jnp.bfloat16)

    for m in range(micro):
        for top in range(cut.late[m], tok, 128):
            rows = cut.rows(first, second, m, top, top + 128)
            normed[m * tok + top : m * tok + top + 128, :] = norm_rows(rows)
        if m == 0:
            queue[-3].start()
    for copy in queue[-2:]:
        copy.start()
    for copy in seconds:
        copy.wait()
    for m in range(micro):
        for top in range(0, cut.late[m], 128):
            rows = norm_rows(cut.rows(first, second, m, top, top + 128))
            normed[m * tok + top : m * tok + top + 128, :] = rows
            low = cut.second_at[m] + top
            second_normed[low : low + 128, :] = rows
    for copy in small:
        copy.wait()
    for number, (part, (weight, kept)) in enumerate(parts.items()):
        loads[part].wait()
        for m in range(micro):
            out = half_silu(dot(normed[m * tok : (m + 1) * tok, :], weight[...]))
            kept[m] = (out * scale if part == 2 else out).astype(jnp.bfloat16)
        if number == 0:
            row = lax.broadcasted_iota(jnp.int32, (tok, 128), 0)
            for m in range(micro):
                low = stream_floors(spans, slot + m, block, alive[slot + m, block], tok)
                own_floors[m] = low
                floors[m] = jnp.maximum(low + tok, row + 1)
                before = alive[slot + m, jnp.maximum(block - 1, 0)]
                counts[m] = jnp.full((8, 128), before, jnp.int32)


def own_kernel(queries, keys, values, own_floors, mixed):
    micro, tok, branch = queries.shape
    pending = []

    def finish(m, head, pieces):
        total = {}
        for (left, right), weights in pieces:
            product = dot(weights, values[m, left:right, lanes(head)])
            for top in range(left, tok, BLOCK):
                piece = product[top - left : top - left + BLOCK]
                total[top] = total[top] + piece if top in total else piece
        mixed[m, :, lanes(head)] = jnp.concatenate([total[t] for t in sorted(total)], 0)

    for m in range(micro):
        masks = {}
        for left, right in local_blocks(0, tok):
            row, col = places(left, tok, left, right)
            masks[left] = (col <= row) & (col >= wide(own_floors[m, left:tok], right - left))
        for head in range(branch // HEAD_DIM):
            pieces = []
            for left, right in local_blocks(0, tok):
                half = dot_rows(queries[m, left:tok, lanes(head)], keys[m, left:right, lanes(head)])
                weights = jnp.where(masks[left], half_silu(half), 0.0).astype(jnp.bfloat16)
                pieces.append(((left, right), weights))
            pending.append((m, head, pieces))
            if len(pending) > 1:
                finish(*pending.pop(0))
    finish(*pending.pop(0))


def far_rows(before, w_kv, keys, values, raw):
    branch = keys.shape[1]
    rows = before.shape[0]
    for top in range(0, rows, BLOCK):
        bottom = min(top + BLOCK, rows)
        normed = before[top:bottom, :]
        if raw:
            normed = normalise(normed.astype(jnp.float32), norm_eps, 0.5).astype(jnp.bfloat16)
        values[top:bottom, :] = half_silu(dot(normed, w_kv[:, :branch])).astype(jnp.bfloat16)
        keys[top:bottom, :] = half_silu(dot(normed, w_kv[:, branch:])).astype(jnp.bfloat16)


def far_sums(low, high, offset, queries, mixed, floors, counts, keys, values, m, at=None):
    blocks = local_blocks(low, high)[::-1]
    edges = sorted({0, *[e for b in blocks for e in b if e > 0]})
    masks = {}
    for left, right in blocks:
        _, col = places(0, right, left, right)
        reach = wide(jnp.concatenate([counts[m]] * (right // 8), 0), right - left)
        masks[left] = (col >= wide(floors[m, 0:right], right - left)) & (col < reach)
    sums = []
    pending = []

    def finish(head, pieces):
        total = {}
        for top, bottom in zip(edges, edges[1:]):
            where = (m, slice(top, bottom)) if at is None else (slice(at + top, at + bottom),)
            total[top] = mixed[(*where, lanes(head))]
        for (left, right), weights in pieces:
            product = dot(weights, values[offset + left : offset + right, lanes(head)])
            for top, bottom in zip(edges, edges[1:]):
                if bottom <= right:
                    total[top] = total[top] + product[top:bottom]
        sums.append(jnp.concatenate([total[t] for t in sorted(total)], 0))

    for head in range(queries.shape[2] // HEAD_DIM):
        pieces = []
        for left, right in blocks:
            half = dot_rows(
                queries[m, 0:right, lanes(head)],
                keys[offset + left : offset + right, lanes(head)],
            )
            weights = jnp.where(masks[left], half_silu(half), 0.0).astype(jnp.bfloat16)
            pieces.append(((left, right), weights))
        pending.append((head, pieces))
        if len(pending) > 1:
            finish(*pending.pop(0))
    finish(*pending.pop(0))
    return sums


def close(sums, top, bottom, x_rows, w_out, gates, m, keep):
    for low in range(top, bottom, BLOCK):
        high = min(low + BLOCK, bottom)
        attended = jnp.concatenate([s[low:high] for s in sums], 1)
        attended = normalise(attended, out_eps * WINDOW)
        gated = (attended * gates[m, low:high, :].astype(jnp.float32)).astype(jnp.bfloat16)
        result = x_rows(m, low, high).astype(jnp.float32) + dot(gated, w_out[...])
        keep(m, low, high, result.astype(jnp.bfloat16))


def far_first_kernel(
    before, first, second, w_kv, w_out, gates, queries, mixed, floors, counts,
    done, rest, keys, values, *, cut,
):
    def keep(m, low, high, result):
        shift = cut.first_at[m] - cut.late[m]
        done[shift + low : shift + high, :] = result

    x_rows = functools.partial(cut.rows, first, second)
    far_rows(before, w_kv, keys, values, True)
    for m in range(cut.micro):
        late = cut.late[m]
        sums = far_sums(
            late, cut.tok, cut.first_at[m] - late, queries, mixed, floors, counts, keys, values, m
        )
        low = cut.second_at[m]
        for head, total in enumerate(sums):
            rest[low : low + late, lanes(head)] = total[:late]
        close(sums, late, cut.tok, x_rows, w_out, gates, m, keep)


def far_second_kernel(
    before, second, w_kv, w_out, gates, queries, rest, floors, counts, first_done,
    out, keys, values, done, sems, *, cut,
):
    copies = []

    def send(source, m, low, high):
        there = out.at[0, m, pl.ds(low, high - low)]
        copies.append(pltpu.make_async_copy(source, there, sems.at[len(copies)]))
        copies[-1].start()

    for m in range(cut.micro):
        rows = cut.tok - cut.late[m]
        send(first_done.at[pl.ds(cut.first_at[m], rows)], m, cut.late[m], cut.tok)

    def keep(m, low, high, result):
        at = cut.second_at[m]
        done[at + low : at + high, :] = result
        send(done.at[pl.ds(at + low, high - low)], m, low, high)

    far_rows(before, w_kv, keys, values, False)
    x_rows = functools.partial(cut.rows, None, second)
    for m in range(cut.micro):
        at = cut.second_at[m]
        sums = far_sums(
            0, cut.late[m], at, queries, rest, floors, counts, keys, values, m, at
        )
        close(sums, 0, cut.late[m], x_rows, w_out, gates, m, keep)
    for copy in copies:
        copy.wait()


VMEM = pl.BlockSpec(memory_space=pltpu.VMEM)
SMEM = pl.BlockSpec(memory_space=pltpu.SMEM)
HBM = pl.BlockSpec(memory_space=pltpu.HBM)


def kept_in_hbm(x):
    return pltpu.with_memory_space_constraint(x, pltpu.HBM)


def layer(x, w_in, w_out, lengths, valid, slot):
    micro, tok, width = x.shape
    branch = w_out.shape[0]
    cut = Cut(micro, tok)
    early, late = cut.first_rows, cut.second_rows
    bf16, f32, i32 = jnp.bfloat16, jnp.float32, jnp.int32
    shape = jax.ShapeDtypeStruct
    params = pltpu.CompilerParams(vmem_limit_bytes=24 << 20)

    def cost(rows, flops, tanhs):
        return pl.CostEstimate(
            flops=rows * flops, transcendentals=rows * tanhs, bytes_accessed=4 << 20
        )

    x = kept_in_hbm(x)
    first = pl.pallas_call(
        functools.partial(cut_kernel, cut=cut),
        out_shape=shape((early, width), bf16),
        in_specs=[HBM],
        out_specs=VMEM,
        scratch_shapes=[pltpu.SemaphoreType.DMA((micro,))],
        compiler_params=params,
        name="cut",
    )(x)
    first_come = shifted(first, "seq", 1)
    fixed = isinstance(slot, int)
    wide_rows = shape((micro, tok, branch), bf16)
    second, second_normed, gates, queries, keys, values, w_kv, own_floors, floors, counts = (
        pl.pallas_call(
            functools.partial(project_kernel, slot, cut=cut)
            if fixed
            else functools.partial(project_kernel_at, cut=cut),
            out_shape=(
                shape((late, width), bf16),
                shape((late, width), bf16),
                *[wide_rows] * 4,
                shape((width, 2 * branch), bf16),
                shape((micro, tok, 128), i32),
                shape((micro, tok, 128), i32),
                shape((micro, 8, 128), i32),
            ),
            in_specs=([] if fixed else [SMEM]) + [VMEM, HBM, HBM, HBM, HBM],
            out_specs=(VMEM,) * 10,
            scratch_shapes=[
                pltpu.VMEM((width, branch), bf16),
                pltpu.VMEM((width, branch), bf16),
                pltpu.VMEM((micro * tok, width), bf16),
                pltpu.SMEM(lengths.shape, i32),
                pltpu.SMEM(valid.shape, i32),
                pltpu.SemaphoreType.DMA((6 + micro,)),
            ],
            compiler_params=params,
            cost_estimate=cost(micro * tok, branch * 8 * width, branch * 4),
            name="project",
        )(*([] if fixed else [slot[None]]), first, x, *map(kept_in_hbm, (w_in, lengths, valid)))
    )
    second_come = shifted(second_normed, "seq", 1)
    mixed = pl.pallas_call(
        own_kernel,
        out_shape=shape((micro, tok, branch), f32),
        in_specs=[VMEM] * 4,
        out_specs=VMEM,
        compiler_params=params,
        cost_estimate=cost(micro * tok, branch * 4 * tok, branch * 2),
        name="own",
    )(queries, keys, values, own_floors)
    first_done, rest = pl.pallas_call(
        functools.partial(far_first_kernel, cut=cut),
        out_shape=(shape((early, width), bf16), shape((late, branch), f32)),
        in_specs=[VMEM] * 10,
        out_specs=(VMEM, VMEM),
        scratch_shapes=[pltpu.VMEM((early, branch), bf16)] * 2,
        compiler_params=params,
        cost_estimate=cost(early, branch * (6 * width + 4 * tok), branch * 4),
        name="far_first",
    )(first_come, first, second, w_kv, w_out, gates, queries, mixed, floors, counts)
    return pl.pallas_call(
        functools.partial(far_second_kernel, cut=cut),
        out_shape=shape((1, micro, tok, width), bf16),
        in_specs=[VMEM] * 10,
        out_specs=HBM,
        scratch_shapes=[
            *[pltpu.VMEM((late, branch), bf16)] * 2,
            pltpu.VMEM((late, width), bf16),
            pltpu.SemaphoreType.DMA((micro * (2 + tok // BLOCK),)),
        ],
        compiler_params=params,
        cost_estimate=cost(late, branch * (6 * width + 4 * tok), branch * 4),
        name="far_second",
    )(second_come, second, w_kv, w_out, gates, queries, rest, floors, counts, first_done)[0]


def project_kernel_at(slot, *refs, cut):
    project_kernel(slot[0], *refs, cut=cut)


def shards(inputs, w_in, w_out, lengths, valid):
    micro, tok, width = inputs.shape
    sections = lax.axis_size("pipe")
    if sections == 1:
        return layer(inputs, w_in[0], w_out[0], lengths, valid, 0)[None]
    section = lax.axis_index("pipe")

    def tick(step, carry):
        incoming, states = carry
        slot = step - section
        active = (slot >= 0) & (slot < micro)
        index = jnp.clip(slot, 0, micro - 1)
        fresh = lax.dynamic_index_in_dim(inputs, index, 0, keepdims=False)
        x_rows = jnp.where(section == 0, fresh, incoming)
        result = layer(x_rows[None], w_in[0], w_out[0], lengths, valid, index)[0]
        updated = lax.dynamic_update_slice(
            states, result[None, None], (jnp.int32(0), index, jnp.int32(0), jnp.int32(0))
        )
        states = jnp.where(active, updated, states)
        return (shifted(result, "pipe", 1), states)

    start_states = jnp.zeros((1, micro, tok, width), jnp.bfloat16)
    start_rows = jnp.zeros((tok, width), jnp.bfloat16)
    _, states = lax.fori_loop(0, sections + micro - 1, tick, (start_rows, start_states))
    return states


def solution(mesh):
    in_specs = (P(None, "seq", None), P("pipe", None, None), P("pipe", None, None), P(), P())
    out_specs = P("pipe", None, "seq", None)
    return jax.shard_map(shards, mesh=mesh, in_specs=in_specs, out_specs=out_specs, check_vma=False)
```
